256 devices in a mesh: lon: 32 (over z, y_hi, core), lat: 8 (over y_lo, x).
Axes of the slice: x: 4, y: 4 (y_hi: 2, y_lo: 2; y = y_hi * 2 + y_lo), z: 8, core: 2. Of those that a mesh axis runs over, the one named last changes fastest.
Arguments:
- fields: bfloat16 [1024, 1024, 256], P('lat', 'lon'), may hold values from -6 to 6
- spec_weight: bfloat16 [2, 2, 17, 256, 256], replicated, may hold values from -0.75 to 0.75
- skip_weight: bfloat16 [2, 256, 256], replicated, may hold values from -0.375 to 0.375
- diffusion: float32 [2, 256], replicated, may hold values from 0.2 to 1
Outputs:
- result: bfloat16 [1024, 1024, 256], P('lat', 'lon')
The draws below stay inside these ranges and needn't reach their ends.
All inputs are finite; a program needn't handle non-finite values.
Results may differ from the reference program's by a relative error of at most 0.01.
Values may be sent and summed in bfloat16 or wider, within the bound.
No kernel may reach another device: no remote copies, remote signals or barrier semaphores. Data moves between devices by JAX's collectives and lax.ppermute only.
A program may use at most 128 MiB of HBM per device.

```python
import math
import jax
import jax.numpy as jnp
from jax import lax

C = 256
WINDOW = 64
HOP = 32
MODES = 17
LAYERS = 2
LAT_DEV = 128
NLAT = 1024
NLON = 1024
N_LAT = 8


def level_of(stream_key, extent, shards, low, largest):
    def one(dim, blocks):
        heights = jax.random.uniform(jax.random.fold_in(jax.random.fold_in(stream_key, 6), dim), (blocks,), jnp.float32, low / len(shards), largest / len(shards))
        return jnp.repeat(jnp.exp(heights), extent[dim] // blocks).reshape((-1,) + (1,) * (len(extent) - dim - 1))

    gain = one(*shards[0])
    for cut in shards[1:]:
        gain = gain * one(*cut)
    return gain


def gaussian(own_key, shape, deviation, most, cuts=(), kind=jnp.bfloat16):
    entries = jax.random.normal(own_key, shape, jnp.float32) * deviation
    if len(cuts) > 0:
        entries = level_of(own_key, shape, cuts, -0.22, 0.18) * entries
    return jnp.clip(entries, min=-most, max=most).astype(kind)


def setup_inputs(seed: int = 0) -> dict:
    key_list = jax.random.split(jax.random.key(seed), 5)
    fields = gaussian(key_list[0], (NLAT, NLON, C), 1.0, 6.0, ((0, 8), (1, 32)))
    spec_weight = gaussian(key_list[1], (LAYERS, 2, MODES, C, C), (C // 4) ** -0.5, 0.75)
    skip_weight = gaussian(key_list[2], (LAYERS, C, C), C ** -0.5, 0.375)
    diffusion = jnp.clip(jnp.exp(jax.random.uniform(key_list[3], (LAYERS, C), jnp.float32, math.log(0.2), math.log(1.0))), 0.2, 1.0)
    return dict(fields=fields, spec_weight=spec_weight, skip_weight=skip_weight, diffusion=diffusion)


def tables(window, mode_count):
    points = jnp.arange(window, dtype=jnp.float32)
    freqs = jnp.arange(mode_count, dtype=jnp.float32)
    angles = 2.0 * math.pi * points[:, None] * freqs[None, :] / window
    taper = 0.5 - 0.5 * jnp.cos(2.0 * math.pi * points / window)
    analysis = jnp.concatenate([taper[:, None] * jnp.cos(angles), -taper[:, None] * jnp.sin(angles)], axis=1).astype(jnp.bfloat16)
    factor = jnp.where(freqs == 0.0, 1.0, 2.0) / window
    synthesis = jnp.concatenate([factor[:, None] * jnp.cos(angles).T, -factor[:, None] * jnp.sin(angles).T], axis=0).astype(jnp.bfloat16)
    return analysis, synthesis


def transform_frames(halves, spec_weight, analysis, synthesis, hop, mode_count):
    halves_wide = halves.astype(jnp.float32)
    front_part = jnp.einsum('lhnc,nj->lhjc', halves_wide, analysis[:hop].astype(jnp.float32))
    back_part = jnp.einsum('lhnc,nj->lhjc', halves_wide, analysis[hop:].astype(jnp.float32))
    coeffs = (front_part[:, :-1] + back_part[:, 1:]).astype(jnp.bfloat16).astype(jnp.float32)
    real_part = coeffs[:, :, :mode_count]
    imag_part = coeffs[:, :, mode_count:]
    weight_real = spec_weight[0].astype(jnp.float32)
    weight_imag = spec_weight[1].astype(jnp.float32)
    mix_real = jnp.einsum('lfkc,kcd->lfkd', real_part, weight_real) - jnp.einsum('lfkc,kcd->lfkd', imag_part, weight_imag)
    mix_imag = jnp.einsum('lfkc,kcd->lfkd', real_part, weight_imag) + jnp.einsum('lfkc,kcd->lfkd', imag_part, weight_real)
    mixed = jnp.concatenate([mix_real, mix_imag], axis=2).astype(jnp.bfloat16).astype(jnp.float32)
    frames_out = jnp.einsum('jn,lfjd->lfnd', synthesis.astype(jnp.float32), mixed)
    return frames_out[:, :, :hop], frames_out[:, :, hop:]


def one_layer(state, layer_spec, layer_skip, layer_diff, analysis, synthesis):
    padded = jnp.pad(state, ((1, 1), (0, 0), (0, 0)))
    frame_count = NLON // HOP

    def band(block):
        start = (block * LAT_DEV).astype(jnp.int32)
        bordered = lax.dynamic_slice_in_dim(padded, start, LAT_DEV + 2, 0)
        centre = bordered[1:-1]
        extended = jnp.concatenate([centre, centre[:, :HOP]], axis=1)
        halves = extended.reshape(LAT_DEV, frame_count + 1, HOP, C)
        first_half, second_half = transform_frames(halves, layer_spec, analysis, synthesis, HOP, MODES)
        spectral = (first_half + jnp.roll(second_half, 1, axis=1)).reshape(LAT_DEV, NLON, C)
        centre_wide = centre.astype(jnp.float32)
        laplacian = bordered[2:].astype(jnp.float32) + bordered[:-2].astype(jnp.float32) - 2.0 * centre_wide
        skipped = jnp.einsum('lwc,cd->lwd', centre_wide, layer_skip.astype(jnp.float32))
        local_term = skipped + layer_diff.astype(jnp.float32) * laplacian
        hidden = spectral + local_term
        return (centre_wide + jax.nn.gelu(hidden)).astype(jnp.bfloat16)

    blocks = lax.map(band, jnp.arange(N_LAT, dtype=jnp.int32))
    return blocks.reshape(NLAT, NLON, C)


def reference(fields, spec_weight, skip_weight, diffusion):
    analysis, synthesis = tables(WINDOW, MODES)
    state = fields
    for layer in range(LAYERS):
        state = one_layer(state, spec_weight[layer], skip_weight[layer], diffusion[layer], analysis, synthesis)
    return state
```

```python
import math

import jax
import jax.numpy as jnp
import ml_dtypes
import numpy as np
from jax import lax
from jax.experimental import pallas as pl
from jax.experimental.pallas import tpu as pltpu
from jax.sharding import PartitionSpec as P

WINDOW = 64
HOP = 32
MODES = 17
COEFS = 2 * MODES
LANE = 8
ROWS = 32
BF16 = jnp.bfloat16
F32 = jnp.float32

CHUNKS = {
    "mid": (10, 12, 12, 8),
    "top": (-2, 12, 0, 12),
    "bot": (22, 12, 20, 12),
}


def tables():
    points = np.arange(WINDOW, dtype=np.float64)
    freqs = np.arange(MODES, dtype=np.float64)
    angles = 2.0 * math.pi * points[:, None] * freqs[None, :] / WINDOW
    taper = 0.5 - 0.5 * np.cos(2.0 * math.pi * points / WINDOW)
    analysis = np.concatenate(
        [taper[:, None] * np.cos(angles), -taper[:, None] * np.sin(angles)], axis=1
    )
    factor = np.where(freqs == 0.0, 1.0, 2.0) / WINDOW
    synthesis = np.concatenate(
        [factor[:, None] * np.cos(angles).T, -factor[:, None] * np.sin(angles).T], axis=0
    )
    return analysis, synthesis


def banded(strips):
    analysis, synthesis = tables()
    frames = strips - 1
    inner = strips - 2
    forward = np.zeros((COEFS, LANE, strips * HOP))
    for f in range(frames):
        forward[:, f, f * HOP : f * HOP + WINDOW] = analysis.T
    backward = np.zeros((inner, HOP, COEFS, LANE))
    for s in range(inner):
        backward[s, :, :, s + 1] = synthesis[:, :HOP].T
        backward[s, :, :, s] = synthesis[:, HOP:].T
    return (
        forward.reshape(COEFS * LANE, strips * HOP).astype(ml_dtypes.bfloat16),
        backward.reshape(inner * HOP, COEFS * LANE).astype(ml_dtypes.bfloat16),
    )


def make_kernel(pieces, in_rows, edge):
    mid_rows = in_rows - 2
    out_rows = in_rows - 4
    n_in = 6 * len(pieces)

    def kernel(info, *refs):
        bufs = refs[:n_in]
        spec, skip, diff, a1, s1, a2, s2 = refs[n_in : n_in + 7]
        outs = refs[n_in + 7 : n_in + 11]
        x, y, o, coef, mixed, w, sem_in, sem_w, sem_out = refs[n_in + 11 :]
        pos = info[0]
        core = info[1]
        base = info[2]

        copies = []
        for p, (row0, rows, at) in enumerate(pieces):
            group = bufs[6 * p : 6 * p + 6]
            places = [(group[m], None, 2 + (pos ^ m)) for m in range(4)]
            for q, start in ((group[4], base), (group[5], 6 - base)):
                places.append((q, 0, start + core))
                places.append((q, 1, start + 1 - core))
            for n, (buf, half, place) in enumerate(places):
                src = buf if half is None else buf.at[half]
                c = pltpu.make_async_copy(
                    src.at[pl.ds(row0, rows)],
                    x.at[pl.ds(at, rows), pl.ds(pl.multiple_of(place * HOP, HOP), HOP)],
                    sem_in.at[p, n],
                )
                c.start()
                copies.append(c)

        def weight(l, k):
            return pltpu.make_async_copy(spec.at[l, :, k], w.at[l, k], sem_w.at[l, k])

        for l in range(2):
            for k in range(MODES):
                weight(l, k).start()
        for c in copies:
            c.wait()

        def layer(l, src, rows, forward, backward, inner, finish):
            def analyse(p, _):
                two = [
                    jnp.dot(forward[...], src[2 * p + 1 + r], preferred_element_type=F32).reshape(
                        COEFS, LANE, 256
                    )
                    for r in range(2)
                ]
                at = pl.multiple_of(p * 2 * LANE, 2 * LANE)
                coef[:, pl.ds(at, 2 * LANE), :] = jnp.concatenate(two, axis=1).astype(BF16)
                return 0

            lax.fori_loop(0, rows // 2, analyse, 0)
            span = rows * LANE

            def mix(k, _):
                weight(l, k).wait()
                re = coef[k, :span]
                im = coef[MODES + k, :span]
                wr = w[l, k, 0]
                wi = w[l, k, 1]
                dot = lambda a, b: jnp.dot(a, b, preferred_element_type=F32)
                mixed[k, :span] = dot(re, wr) - dot(im, wi)
                mixed[MODES + k, :span] = dot(re, wi) + dot(im, wr)
                return 0

            lax.fori_loop(0, MODES, mix, 0)
            wide = inner * HOP

            def synth(r, _):
                at = pl.multiple_of(r * LANE, LANE)
                rhs = mixed[:, pl.ds(at, LANE), :].reshape(COEFS * LANE, 256).astype(BF16)
                spectral = jnp.dot(backward[...], rhs, preferred_element_type=F32)
                mid = src[r + 1, HOP : HOP + wide]
                skipped = jnp.dot(mid, skip[l], preferred_element_type=F32)
                mid = mid.astype(F32)
                up = src[r, HOP : HOP + wide].astype(F32)
                down = src[r + 2, HOP : HOP + wide].astype(F32)
                lap = down + up - 2.0 * mid
                hidden = spectral + (skipped + diff[l : l + 1] * lap)
                finish(r, mid + jax.nn.gelu(hidden))
                return 0

            lax.fori_loop(0, rows, synth, 0)

        def first(r, value):
            y[r] = value.astype(BF16)

        layer(0, x, mid_rows, a1, s1, 6, first)

        if edge:
            row = 0 if edge < 0 else mid_rows - 1

            @pl.when(info[3 if edge < 0 else 4] == 1)
            def _():
                y[row] = jnp.zeros_like(y[row])

        def second(r, value):
            o[r] = value.astype(BF16)

        layer(1, y, out_rows, a2, s2, 4, second)

        done = []
        for m in range(4):
            c = pltpu.make_async_copy(
                o.at[:, pl.ds(pl.multiple_of((pos ^ m) * HOP, HOP), HOP)], outs[m], sem_out.at[m]
            )
            c.start()
            done.append(c)
        for c in done:
            c.wait()

    any_ = pl.BlockSpec(memory_space=pl.ANY)
    vmem = pl.BlockSpec(memory_space=pltpu.VMEM)
    return pl.pallas_call(
        kernel,
        out_shape=[jax.ShapeDtypeStruct((out_rows, HOP, 256), BF16)] * 4,
        in_specs=[pl.BlockSpec(memory_space=pltpu.SMEM)] + [any_] * n_in + [any_] + [vmem] * 6,
        out_specs=[any_] * 4,
        scratch_shapes=[
            pltpu.VMEM((in_rows, 8 * HOP, 256), BF16),
            pltpu.VMEM((mid_rows, 6 * HOP, 256), BF16),
            pltpu.VMEM((out_rows, 4 * HOP, 256), BF16),
            pltpu.VMEM((COEFS, mid_rows * LANE, 256), BF16),
            pltpu.VMEM((COEFS, mid_rows * LANE, 256), F32),
            pltpu.VMEM((2, MODES, 2, 256, 256), BF16),
            pltpu.SemaphoreType.DMA((len(pieces), 8)),
            pltpu.SemaphoreType.DMA((2, MODES)),
            pltpu.SemaphoreType.DMA((4,)),
        ],
        compiler_params=pltpu.CompilerParams(vmem_limit_bytes=40 << 20),
        name="layers",
    )


def local(fields, spec_weight, skip_weight, diffusion):
    lon = lax.axis_index("lon")
    lat = lax.axis_index("lat")
    n_lon = lax.axis_size("lon")
    n_lat = lax.axis_size("lat")
    pos = lon % 4

    def swap(v, m):
        return lax.ppermute(v, "lon", [(i, i ^ m) for i in range(n_lon)])

    def along(v, low, high):
        return lax.ppermute(
            v, "lon", [(i, (i + (low if i % 4 < 2 else high)) % n_lon) for i in range(n_lon)]
        )

    above = lax.ppermute(fields[-2:], "lat", [(i, i + 1) for i in range(n_lat - 1)])
    below = lax.ppermute(fields[:2], "lat", [(i + 1, i) for i in range(n_lat - 1)])
    bordered = jnp.concatenate([above, fields, below], axis=0)

    def gather(name):
        first, rows = CHUNKS[name][:2]
        source, shift = (fields, first) if name == "mid" else (bordered, first + 2)
        got = []
        for m in range(4):
            piece = lax.dynamic_slice_in_dim(source, (pos ^ m) * ROWS + shift, rows, 0)
            got.append(swap(piece, m) if m else piece)
        near = along(jnp.stack(got[:2]), -4, 4)
        far = along(jnp.stack(got[2:]), 4, -4)
        return got + [near, far]

    info = jnp.stack(
        [
            pos,
            pos % 2,
            jnp.where(pos < 2, 6, 0),
            ((lat == 0) & (pos == 0)).astype(jnp.int32),
            ((lat == n_lat - 1) & (pos == 3)).astype(jnp.int32),
        ]
    ).astype(jnp.int32)
    a1, s1 = banded(8)
    a2, s2 = banded(6)
    rest = (spec_weight, skip_weight, diffusion, a1, s1, a2, s2)

    mid = gather("mid")
    top = gather("top")
    bot = gather("bot")
    outs = {}
    outs["mid"] = make_kernel([(0, 12, 0)], 12, 0)(info, *mid, *rest)
    outs["top"] = make_kernel([(0, 12, 0), (0, 4, 12)], 16, -1)(info, *top, *mid, *rest)
    outs["bot"] = make_kernel([(8, 4, 0), (0, 12, 4)], 16, 1)(info, *mid, *bot, *rest)
    result = jnp.zeros(fields.shape, BF16)
    for name in ("mid", "top", "bot"):
        start = CHUNKS[name][2]
        for m in range(4):
            piece = swap(outs[name][m], m) if m else outs[name][m]
            result = lax.dynamic_update_slice_in_dim(result, piece, (pos ^ m) * ROWS + start, 0)
    return result


def solution(mesh):
    in_specs = (P("lat", "lon", None), P(), P(), P())
    out_specs = P("lat", "lon", None)
    return jax.shard_map(local, mesh=mesh, in_specs=in_specs, out_specs=out_specs, check_vma=False)
```

```python
import math

import jax
import jax.numpy as jnp
import ml_dtypes
import numpy as np
from jax import lax
from jax.experimental import pallas as pl
from jax.experimental.pallas import tpu as pltpu
from jax.sharding import PartitionSpec as P

WINDOW = 64
HOP = 32
MODES = 17
COEFS = 2 * MODES
LANE = 8

BF16 = jnp.bfloat16
F32 = jnp.float32
GELU_A = 2.0 * math.sqrt(2.0 / math.pi)
GELU_B = 4.0 * 0.044715 * GELU_A
VMEM_LIMIT = 14 << 20
ROWS = 32

TAKE = {"mid": (10, 12), "top": (-2, 12), "bot": (22, 12)}
CHUNKS = {
    "mid": (12, [("mid", 0, 12)]),
    "top": (0, [("top", 0, 12), ("mid", 0, 4)]),
    "bot": (20, [("mid", 8, 4), ("bot", 0, 12)]),
}


def tables():
    points = np.arange(WINDOW, dtype=np.float64)
    freqs = np.arange(MODES, dtype=np.float64)
    angles = 2.0 * math.pi * points[:, None] * freqs[None, :] / WINDOW
    taper = 0.5 - 0.5 * np.cos(2.0 * math.pi * points / WINDOW)
    analysis = np.concatenate(
        [taper[:, None] * np.cos(angles), -taper[:, None] * np.sin(angles)], axis=1
    )
    factor = np.where(freqs == 0.0, 1.0, 2.0) / WINDOW
    synthesis = np.concatenate(
        [factor[:, None] * np.cos(angles).T, -factor[:, None] * np.sin(angles).T], axis=0
    )
    return analysis, synthesis


def banded(sources, places):
    analysis, synthesis = tables()
    strips = len(sources)
    forward = np.zeros((COEFS, LANE, strips, HOP))
    for n, s in enumerate(sources):
        if s < strips - 1:
            forward[:, s, n] = analysis[:HOP].T
        if s > 0:
            forward[:, s - 1, n] = analysis[HOP:].T
    backward = np.zeros((len(places), HOP, 2, MODES, LANE))
    for n, s in enumerate(places):
        backward[n, :, :, :, s] = synthesis[:, :HOP].T.reshape(HOP, 2, MODES)
        backward[n, :, :, :, s - 1] = synthesis[:, HOP:].T.reshape(HOP, 2, MODES)
    backward = backward.transpose(0, 1, 3, 2, 4)
    return (
        forward.reshape(COEFS * LANE, strips * HOP).astype(ml_dtypes.bfloat16),
        0.5 * backward.reshape(len(places) * HOP, COEFS * LANE).astype(ml_dtypes.bfloat16),
    )


def all_tables():
    sets = []
    for own, other, near, far in ((2, 4, 6, 0), (4, 2, 0, 6)):
        first = [p + n for p in (own, other, near, far) for n in range(2)]
        inner = first[:4] + [6 if p else 1 for p in (near, far)]
        second = [p - 1 for p in inner]
        sets.append(banded(first, inner) + banded(second, second[:4]))
    return [np.stack(t) for t in zip(*sets)]


def make_kernel(place, n_in, edge):
    in_rows = len(place)
    mid_rows = in_rows - 2
    out_rows = in_rows - 4

    def kernel(info, *refs):
        bufs = refs[:n_in]
        spec, skip, diff, a1, s1, a2, s2 = refs[n_in : n_in + 7]
        outs = refs[n_in + 7 : n_in + 11]
        y, coef, mixed = refs[n_in + 11 :]
        high = info[0]
        core = info[1]
        near_inner = info[2]
        far_inner = info[3]

        def strips(row, *wanted):
            return [bufs[place[row][b][0]][e, place[row][b][1]] for b, e in wanted]

        evens = [(b, e) for b in range(4) for e in (core, 1 - core)]

        def window(row):
            return jnp.concatenate(strips(row, *evens), axis=0)

        def inner(row):
            return jnp.concatenate(
                strips(row, *evens[:4], (2, near_inner), (3, far_inner)), axis=0
            )

        def analyse(forward, get, rows):
            for r in range(0, rows, 2):
                two = [
                    jnp.dot(forward[high], get(r + n), preferred_element_type=F32).reshape(
                        COEFS, LANE, 256
                    )
                    for n in range(2)
                ]
                coef[:, r * LANE : (r + 2) * LANE, :] = jnp.concatenate(two, axis=1).astype(BF16)

        def mix(l, rows):
            span = rows * LANE
            for k in range(MODES):
                re = coef[k, :span]
                im = coef[MODES + k, :span]
                wr = spec[l, 0, k]
                wi = spec[l, 1, k]
                parts = [
                    jnp.dot(
                        jnp.concatenate([re, i], axis=1),
                        jnp.concatenate(ws, axis=0),
                        preferred_element_type=F32,
                    ).reshape(rows, LANE, 256)
                    for i, ws in ((-im, (wr, wi)), (im, (wi, wr)))
                ]
                mixed[:rows, k * 2 * LANE : (k + 1) * 2 * LANE, :] = jnp.concatenate(
                    parts, axis=1
                ).astype(BF16)

        def synth(l, backward, get, rows, finish):
            lines = [get(r) for r in range(2)]
            wide = [v.astype(F32) for v in lines]
            for r in range(rows):
                lines.append(get(r + 2))
                wide.append(lines[r + 2].astype(F32))
                mid = wide[r + 1]
                total = jnp.dot(
                    jnp.concatenate([lines[r + 1], backward[high]], axis=1),
                    jnp.concatenate([skip[l], mixed[r]], axis=0),
                    preferred_element_type=F32,
                )
                half = total + diff[l : l + 1] * ((wide[r] - mid) + (wide[r + 2] - mid))
                inside = half * (GELU_A + GELU_B * (half * half))
                finish(r, ((mid + half) + half * jnp.tanh(inside)).astype(BF16))

        def first(r, value):
            y[r] = value

        def second(r, value):
            lower = core == 0
            for p in range(2):
                even = value[2 * p * HOP : (2 * p + 1) * HOP]
                odd = value[(2 * p + 1) * HOP : (2 * p + 2) * HOP]
                outs[2 * p][r] = jnp.where(lower, even, odd)
                outs[2 * p + 1][r] = jnp.where(lower, odd, even)

        analyse(a1, lambda r: window(r + 1), mid_rows)
        mix(0, mid_rows)
        synth(0, s1, inner, mid_rows, first)

        if edge:
            row = 0 if edge < 0 else mid_rows - 1

            @pl.when(info[4 if edge < 0 else 5] == 1)
            def _():
                y[row] = jnp.zeros((6 * HOP, 256), BF16)

        analyse(a2, lambda r: y[r + 1], out_rows)
        mix(1, out_rows)
        synth(1, s2, lambda r: y[r][: 4 * HOP], out_rows, second)

    vmem = pl.BlockSpec(memory_space=pltpu.VMEM)
    frames = 7 * mid_rows + 5 * out_rows
    return pl.pallas_call(
        kernel,
        out_shape=[jax.ShapeDtypeStruct((out_rows, HOP, 256), BF16)] * 4,
        in_specs=[pl.BlockSpec(memory_space=pltpu.SMEM)] + [vmem] * (n_in + 7),
        out_specs=[vmem] * 4,
        scratch_shapes=[
            pltpu.VMEM((mid_rows, 6 * HOP, 256), BF16),
            pltpu.VMEM((COEFS, mid_rows * LANE, 256), BF16),
            pltpu.VMEM((mid_rows, COEFS * LANE, 256), BF16),
        ],
        compiler_params=pltpu.CompilerParams(vmem_limit_bytes=VMEM_LIMIT),
        cost_estimate=pl.CostEstimate(
            flops=frames * (MODES * 8 * 256 * 256 + 2 * COEFS * (WINDOW + HOP) * 256),
            transcendentals=(mid_rows * 6 + out_rows * 4) * HOP * 256,
            bytes_accessed=in_rows * 8 * HOP * 256 * 2,
        ),
        name="layers",
    )


def local(fields, spec_weight, skip_weight, diffusion):
    lon = lax.axis_index("lon")
    lat = lax.axis_index("lat")
    n_lon = lax.axis_size("lon")
    n_lat = lax.axis_size("lat")
    pos = lon % 4
    core = pos % 2

    def swap(v, m):
        return lax.ppermute(v, "lon", [(i, i ^ m) for i in range(n_lon)])

    def along(v, low, high):
        return lax.ppermute(
            v, "lon", [(i, (i + (low if i % 4 < 2 else high)) % n_lon) for i in range(n_lon)]
        )

    above = lax.ppermute(fields[-2:], "lat", [(i, i + 1) for i in range(n_lat - 1)])
    below = lax.ppermute(fields[:2], "lat", [(i + 1, i) for i in range(n_lat - 1)])
    ends = {
        "top": (0, jnp.concatenate([above, fields[:10]], axis=0)),
        "bot": (3, jnp.concatenate([fields[-10:], below], axis=0)),
    }

    def piece(name, m):
        shift, rows = TAKE[name]
        block = pos ^ m
        got = lax.dynamic_slice_in_dim(fields, block * ROWS + shift, rows, 0)
        if name in ends:
            where, other = ends[name]
            got = jnp.where(block == where, other, got)
        return got

    def own_pair(names):
        mine, his = (jnp.concatenate([piece(n, m) for n in names], axis=0) for m in (0, 1))
        return jnp.stack([mine, swap(his, 1)])

    def other_pair(name):
        return [swap(piece(name, m), m) for m in (2, 3)]

    sets = {}
    raw = {"mid": other_pair("mid")}
    own_mid = own_pair(["mid"])
    raw["top"] = other_pair("top")
    raw["bot"] = other_pair("bot")
    own_ends = own_pair(["top", "bot"])
    near_mid = along(own_mid, -4, 4)
    near_ends = along(own_ends, -4, 4)
    for name, own, near, at in (
        ("mid", own_mid, near_mid, 0),
        ("top", own_ends, near_ends, 0),
        ("bot", own_ends, near_ends, 12),
    ):
        other = jnp.stack(raw[name])
        far = along(other, 4, -4)
        sets[name] = ((own, at), (other, 0), (near, at), (far, 0))

    info = jnp.stack(
        [
            pos // 2,
            core,
            jnp.where(pos < 2, core, 1 - core),
            jnp.where(pos < 2, 1 - core, core),
            ((lat == 0) & (pos == 0)).astype(jnp.int32),
            ((lat == n_lat - 1) & (pos == 3)).astype(jnp.int32),
        ]
    ).astype(jnp.int32)
    rest = (spec_weight, 0.5 * skip_weight, 0.5 * diffusion, *all_tables())

    result = jnp.zeros(fields.shape, BF16)
    for name, edge in (("mid", 0), ("top", -1), ("bot", 1)):
        start, parts = CHUNKS[name]
        arrays, place = [], []
        for part, row0, rows in parts:
            index = []
            for array, _ in sets[part]:
                index.append(len(arrays))
                arrays.append(array)
            for r in range(rows):
                place.append([(i, at + row0 + r) for i, (_, at) in zip(index, sets[part])])
        outs = make_kernel(place, len(arrays), edge)(info, *arrays, *rest)
        for m in range(4):
            back = swap(outs[m], m) if m else outs[m]
            result = lax.dynamic_update_slice_in_dim(result, back, (pos ^ m) * ROWS + start, 0)
    return result


def solution(mesh):
    in_specs = (P("lat", "lon", None), P(), P(), P())
    out_specs = P("lat", "lon", None)
    return jax.shard_map(local, mesh=mesh, in_specs=in_specs, out_specs=out_specs, check_vma=False)
```

```python
import math

import jax
import jax.numpy as jnp
import ml_dtypes
import numpy as np
from jax import lax
from jax.experimental import pallas as pl
from jax.experimental.pallas import tpu as pltpu
from jax.sharding import PartitionSpec as P


WINDOW = 64
HOP = 32
MODES = 17
COEFS = 2 * MODES
LANE = 8

BF16 = jnp.bfloat16
F32 = jnp.float32
GELU_A = 2.0 * math.sqrt(2.0 / math.pi)
GELU_B = 4.0 * 0.044715 * GELU_A
VMEM_LIMIT = 16 << 20
SMALL_LIMIT = 4 << 20
CUT_FLOPS = 1 << 31
ROWS = 32

MID = (6, 20)
END = 8


def tables():
    points = np.arange(WINDOW, dtype=np.float64)
    freqs = np.arange(MODES, dtype=np.float64)
    angles = 2.0 * math.pi * points[:, None] * freqs[None, :] / WINDOW
    taper = 0.5 - 0.5 * np.cos(2.0 * math.pi * points / WINDOW)
    analysis = np.concatenate(
        [taper[:, None] * np.cos(angles), -taper[:, None] * np.sin(angles)], axis=1
    )
    factor = np.where(freqs == 0.0, 1.0, 2.0) / WINDOW
    synthesis = np.concatenate(
        [factor[:, None] * np.cos(angles).T, -factor[:, None] * np.sin(angles).T], axis=0
    )
    return analysis, synthesis


def banded(sources, places):
    analysis, synthesis = tables()
    strips = len(sources)
    forward = np.zeros((COEFS, LANE, strips, HOP))
    for n, s in enumerate(sources):
        if s < strips - 1:
            forward[:, s, n] = analysis[:HOP].T
        if s > 0:
            forward[:, s - 1, n] = analysis[HOP:].T
    backward = np.zeros((len(places), HOP, 2, MODES, LANE))
    for n, s in enumerate(places):
        backward[n, :, :, :, s] = synthesis[:, :HOP].T.reshape(HOP, 2, MODES)
        backward[n, :, :, :, s - 1] = synthesis[:, HOP:].T.reshape(HOP, 2, MODES)
    backward = backward.transpose(0, 1, 3, 2, 4)
    return (
        forward.reshape(COEFS * LANE, strips * HOP).astype(ml_dtypes.bfloat16),
        (0.5 * backward.reshape(len(places) * HOP, COEFS * LANE)).astype(ml_dtypes.bfloat16),
    )


def all_tables():
    sets = []
    for own, other, near, far in ((2, 4, 6, 0), (4, 2, 0, 6)):
        first = [p + n for p in (own, other, near, far) for n in range(2)]
        inner = first[:4] + [6 if p else 1 for p in (near, far)]
        second = [p - 1 for p in inner]
        sets.append(banded(first, inner) + banded(second, second[:4]))
    return [np.stack(t) for t in zip(*sets)]


def make_kernel(runs, n_in, edges):
    mid_rows = sum(len(run) - 2 for run in runs)
    out_rows = sum(len(run) - 4 for run in runs)

    def spans(cut):
        at = 0
        for run in runs:
            yield run, at, len(run) - cut
            at += len(run) - cut

    def kernel(info, *refs):
        bufs = refs[:n_in]
        spec, skip, diff, a1, s1, a2, s2 = refs[n_in : n_in + 7]
        outs = refs[n_in + 7 : n_in + 11]
        y, coef, mixed = refs[n_in + 11 :]
        high = info[0]
        core = info[1]
        near_inner = info[2]
        far_inner = info[3]

        def strips(row, *wanted):
            return [bufs[row[b][0]][e, row[b][1]] for b, e in wanted]

        evens = [(b, e) for b in range(4) for e in (core, 1 - core)]

        def window(row):
            return jnp.concatenate(strips(row, *evens), axis=0)

        def inner(row):
            return jnp.concatenate(
                strips(row, *evens[:4], (2, near_inner), (3, far_inner)), axis=0
            )

        def analyse(forward, rows):
            for r in range(0, len(rows), 2):
                two = [
                    jnp.dot(forward[high], get(), preferred_element_type=F32).reshape(
                        COEFS, LANE, 256
                    )
                    for get in rows[r : r + 2]
                ]
                coef[:, r * LANE : (r + 2) * LANE, :] = jnp.concatenate(two, axis=1).astype(BF16)

        def mix(l, rows):
            span = rows * LANE
            for k in range(MODES):
                re = coef[k, :span]
                im = coef[MODES + k, :span]
                wr = spec[l, 0, k]
                wi = spec[l, 1, k]
                parts = [
                    jnp.dot(
                        jnp.concatenate([re, i], axis=1),
                        jnp.concatenate(ws, axis=0),
                        preferred_element_type=F32,
                    ).reshape(rows, LANE, 256)
                    for i, ws in ((-im, (wr, wi)), (im, (wi, wr)))
                ]
                mixed[:rows, k * 2 * LANE : (k + 1) * 2 * LANE, :] = jnp.concatenate(
                    parts, axis=1
                ).astype(BF16)

        def synth(l, backward, get, at, rows, finish):
            local = skip[l] * 0.5
            spread = diff[l : l + 1] * 0.5
            lines = [get(r) for r in range(2)]
            wide = [v.astype(F32) for v in lines]
            for r in range(rows):
                lines.append(get(r + 2))
                wide.append(lines[r + 2].astype(F32))
                mid = wide[r + 1]
                total = jnp.dot(
                    jnp.concatenate([lines[r + 1], backward[high]], axis=1),
                    jnp.concatenate([local, mixed[at + r]], axis=0),
                    preferred_element_type=F32,
                )
                half = total + spread * ((wide[r] - mid) + (wide[r + 2] - mid))
                inside = half * (GELU_A + GELU_B * (half * half))
                finish(at + r, ((mid + half) + half * jnp.tanh(inside)).astype(BF16))

        def first(r, value):
            y[r] = value

        def second(r, value):
            lower = core == 0
            for p in range(2):
                even = value[2 * p * HOP : (2 * p + 1) * HOP]
                odd = value[(2 * p + 1) * HOP : (2 * p + 2) * HOP]
                outs[2 * p][r] = jnp.where(lower, even, odd)
                outs[2 * p + 1][r] = jnp.where(lower, odd, even)

        analyse(a1, [lambda row=row: window(row) for run in runs for row in run[1:-1]])
        mix(0, mid_rows)
        for run, at, rows in spans(2):
            synth(0, s1, lambda r, run=run: inner(run[r]), at, rows, first)

        if edges:
            for n, row in enumerate((0, mid_rows - 1)):

                @pl.when(info[4 + n] == 1)
                def _(row=row):
                    y[row] = jnp.zeros((6 * HOP, 256), BF16)

        inside = [at + r for _, at, rows in spans(2) for r in range(1, rows - 1)]
        analyse(a2, [lambda r=r: y[r] for r in inside])
        mix(1, out_rows)
        for (_, at, rows), (_, start, _) in zip(spans(4), spans(2)):
            synth(1, s2, lambda r, start=start: y[start + r][: 4 * HOP], at, rows, second)

    vmem = pl.BlockSpec(memory_space=pltpu.VMEM)
    frames = 7 * mid_rows + 5 * out_rows
    return pl.pallas_call(
        kernel,
        out_shape=[jax.ShapeDtypeStruct((out_rows, HOP, 256), BF16)] * 4,
        in_specs=[pl.BlockSpec(memory_space=pltpu.SMEM)] + [vmem] * (n_in + 7),
        out_specs=[vmem] * 4,
        scratch_shapes=[
            pltpu.VMEM((mid_rows, 6 * HOP, 256), BF16),
            pltpu.VMEM((COEFS, mid_rows * LANE, 256), BF16),
            pltpu.VMEM((mid_rows, COEFS * LANE, 256), BF16),
        ],
        compiler_params=pltpu.CompilerParams(vmem_limit_bytes=VMEM_LIMIT),
        cost_estimate=pl.CostEstimate(
            flops=frames * (MODES * 8 * 256 * 256 + 2 * COEFS * (WINDOW + HOP) * 256),
            transcendentals=(mid_rows * 6 + out_rows * 4) * HOP * 256,
            bytes_accessed=mid_rows * 8 * HOP * 256 * 2,
        ),
        name="layers",
    )


def cut_middle(info, fields):
    shift, rows = MID

    def kernel(info, fields, *refs):
        outs, sem = refs[:6], refs[6]
        pos = info[0]
        copies = []
        for n, m in enumerate((2, 3, 1, 0)):
            src = fields.at[pl.ds((pos ^ m) * ROWS + shift, rows)]
            copies.append(pltpu.make_async_copy(src, outs[m], sem.at[n]))
        copies.append(pltpu.make_async_copy(fields.at[pl.ds(126, 2)], outs[4], sem.at[4]))
        copies.append(pltpu.make_async_copy(fields.at[pl.ds(0, 2)], outs[5], sem.at[5]))
        for c in copies:
            c.start()
        for c in copies:
            c.wait()

    vmem = pl.BlockSpec(memory_space=pltpu.VMEM)
    piece = jax.ShapeDtypeStruct((rows, HOP, 256), BF16)
    edge = jax.ShapeDtypeStruct((2, HOP, 256), BF16)
    return pl.pallas_call(
        kernel,
        out_shape=[piece] * 4 + [edge] * 2,
        in_specs=[
            pl.BlockSpec(memory_space=pltpu.SMEM),
            pl.BlockSpec(memory_space=pltpu.HBM),
        ],
        out_specs=[vmem] * 6,
        scratch_shapes=[pltpu.SemaphoreType.DMA((6,))],
        cost_estimate=pl.CostEstimate(flops=CUT_FLOPS, transcendentals=0, bytes_accessed=1 << 20),
        compiler_params=pltpu.CompilerParams(vmem_limit_bytes=SMALL_LIMIT),
        name="cut_middle",
    )(info, fields)


def cut_ends(info, fields, above, below):
    def kernel(info, fields, above, below, *refs):
        outs, sem = refs[:4], refs[4]
        pos = info[0]
        waits = []
        for m in (2, 3, 1, 0):
            block = pos ^ m
            start = block * ROWS
            out = outs[m]
            for n, (at, src, edge, beyond, other, last) in enumerate(
                (
                    (2, start, 0, start - 2, above, 0),
                    (END, start + ROWS - END + 2, 2 * END - 2, start + ROWS, below, 3),
                )
            ):
                c = pltpu.make_async_copy(
                    fields.at[pl.ds(src, END - 2)], out.at[pl.ds(at, END - 2)], sem.at[m, n, 0]
                )
                c.start()
                rim = out.at[pl.ds(edge, 2)]
                got = pltpu.make_async_copy(other, rim, sem.at[m, n, 1])

                @pl.when(block == last)
                def _(got=got):
                    got.start()

                @pl.when(block != last)
                def _(beyond=beyond, rim=rim, m=m, n=n):
                    pltpu.make_async_copy(
                        fields.at[pl.ds(beyond, 2)], rim, sem.at[m, n, 1]
                    ).start()

                waits += [c, got]
        for c in waits:
            c.wait()

    vmem = pl.BlockSpec(memory_space=pltpu.VMEM)
    piece = jax.ShapeDtypeStruct((2 * END, HOP, 256), BF16)
    return pl.pallas_call(
        kernel,
        out_shape=[piece] * 4,
        in_specs=[
            pl.BlockSpec(memory_space=pltpu.SMEM),
            pl.BlockSpec(memory_space=pltpu.HBM),
            pl.BlockSpec(memory_space=pl.ANY),
            pl.BlockSpec(memory_space=pl.ANY),
        ],
        out_specs=[vmem] * 4,
        scratch_shapes=[pltpu.SemaphoreType.DMA((4, 2, 2))],
        cost_estimate=pl.CostEstimate(flops=CUT_FLOPS, transcendentals=0, bytes_accessed=1 << 20),
        compiler_params=pltpu.CompilerParams(vmem_limit_bytes=SMALL_LIMIT),
        name="cut_ends",
    )(info, fields, above, below)


def paste(info, pieces, spots, result=None):
    def kernel(info, *refs):
        out, sem = refs[-2], refs[-1]
        copies = []
        for m in range(4):
            for n, (row, count, at) in enumerate(spots):
                dst = out.at[pl.ds((info[0] ^ m) * ROWS + at, count)]
                copies.append(
                    pltpu.make_async_copy(refs[m].at[pl.ds(row, count)], dst, sem.at[m, n])
                )
        for c in copies:
            c.start()
        for c in copies:
            c.wait()

    some = pl.BlockSpec(memory_space=pl.ANY)
    hbm = pl.BlockSpec(memory_space=pltpu.HBM)
    more = () if result is None else (result,)
    return pl.pallas_call(
        kernel,
        out_shape=jax.ShapeDtypeStruct((4 * ROWS, HOP, 256), BF16),
        in_specs=[pl.BlockSpec(memory_space=pltpu.SMEM)] + [some] * 4 + [hbm] * len(more),
        out_specs=hbm,
        input_output_aliases={5: 0} if more else {},
        scratch_shapes=[pltpu.SemaphoreType.DMA((4, len(spots)))],
        compiler_params=pltpu.CompilerParams(vmem_limit_bytes=SMALL_LIMIT),
        name="paste",
    )(info, *pieces, *more)


def load(spec_weight, skip_weight, diffusion, *tables):
    sources = (spec_weight, skip_weight, diffusion, *tables)
    count = len(sources)

    def kernel(*refs):
        sem = refs[2 * count]
        copies = [
            pltpu.make_async_copy(src, dst, sem.at[n])
            for n, (src, dst) in enumerate(zip(refs[:count], refs[count : 2 * count]))
        ]
        for c in copies:
            c.start()
        for c in copies:
            c.wait()

    return pl.pallas_call(
        kernel,
        out_shape=[pltpu.VMEM(v.shape, v.dtype) for v in sources],
        in_specs=[pl.BlockSpec(memory_space=pltpu.HBM)] * count,
        out_specs=[pl.BlockSpec(memory_space=pltpu.VMEM)] * count,
        scratch_shapes=[pltpu.SemaphoreType.DMA((count,))],
        compiler_params=pltpu.CompilerParams(vmem_limit_bytes=SMALL_LIMIT),
        name="load",
    )(*(pltpu.with_memory_space_constraint(v, pltpu.HBM) for v in sources))


def program(fields, spec_weight, skip_weight, diffusion):
    lon = lax.axis_index("lon")
    lat = lax.axis_index("lat")
    n_lon = lax.axis_size("lon")
    n_lat = lax.axis_size("lat")
    pos = lon % 4
    core = pos % 2

    def swap(v, m):
        return lax.ppermute(v, "lon", [(i, i ^ m) for i in range(n_lon)])

    def along(v, low, high):
        pairs = [(i, (i + (low if i % 4 < 2 else high)) % n_lon) for i in range(n_lon)]
        return lax.ppermute(v, "lon", pairs)

    info = jnp.stack(
        [
            pos // 2,
            core,
            jnp.where(pos < 2, core, 1 - core),
            jnp.where(pos < 2, 1 - core, core),
            ((lat == 0) & (pos == 0)).astype(jnp.int32),
            ((lat == n_lat - 1) & (pos == 3)).astype(jnp.int32),
        ]
    ).astype(jnp.int32)
    at = pos.astype(jnp.int32).reshape(1)

    own, one, two, three, tail, head = cut_middle(at, fields)
    above = lax.ppermute(tail, "lat", [(i, i + 1) for i in range(n_lat - 1)])
    below = lax.ppermute(head, "lat", [(i + 1, i) for i in range(n_lat - 1)])
    other_mid = jnp.stack([swap(two, 2), swap(three, 3)])
    own_mid = jnp.stack([own, swap(one, 1)])
    near_mid = along(own_mid, -4, 4)
    far_mid = along(other_mid, 4, -4)

    own, one, two, three = cut_ends(at, fields, above, below)
    other_end = jnp.stack([swap(two, 2), swap(three, 3)])
    own_end = jnp.stack([own, swap(one, 1)])
    near_end = along(own_end, -4, 4)
    far_end = along(other_end, 4, -4)

    mid = (own_mid, other_mid, near_mid, far_mid)
    end = (own_end, other_end, near_end, far_end)
    rest = load(spec_weight, skip_weight, diffusion, *map(jnp.asarray, all_tables()))

    def rows(first, start, count):
        return [[(first + b, r) for b in range(4)] for r in range(start, start + count)]

    outs = make_kernel([rows(0, 0, MID[1])], 4, False)(info, *mid, *rest)
    back_mid = [swap(outs[m], m) if m else outs[m] for m in range(4)]
    runs = [rows(0, 0, END) + rows(4, 0, 4), rows(4, MID[1] - 4, 4) + rows(0, END, END)]
    outs = make_kernel(runs, 8, True)(info, *end, *mid, *rest)
    back_end = [swap(outs[m], m) if m else outs[m] for m in range(4)]

    result = paste(at, back_mid, [(0, ROWS - 2 * END, END)])
    result = paste(at, back_end, [(0, END, 0), (END, END, ROWS - END)], result)
    return result


def solution(mesh):
    in_specs = (P("lat", "lon", None), P(), P(), P())
    out_specs = P("lat", "lon", None)
    return jax.shard_map(program, mesh=mesh, in_specs=in_specs, out_specs=out_specs, check_vma=False)
```

```python
import math

import jax
import jax.numpy as jnp
import ml_dtypes
import numpy as np
from jax import lax
from jax.experimental import pallas as pl
from jax.experimental.pallas import tpu as pltpu
from jax.sharding import PartitionSpec as P


WINDOW = 64
HOP = 32
MODES = 17
COEFS = 2 * MODES
LANE = 8

BF16 = jnp.bfloat16
F32 = jnp.float32
GELU_A = 2.0 * math.sqrt(2.0 / math.pi)
GELU_B = 4.0 * 0.044715 * GELU_A
VMEM_LIMIT = 16 << 20
SMALL_LIMIT = 4 << 20
CUT_FLOPS = 1 << 31
ROWS = 32

MID = (6, 20)
END = 8


def tables():
    points = np.arange(WINDOW, dtype=np.float64)
    freqs = np.arange(MODES, dtype=np.float64)
    angles = 2.0 * math.pi * points[:, None] * freqs[None, :] / WINDOW
    taper = 0.5 - 0.5 * np.cos(2.0 * math.pi * points / WINDOW)
    analysis = np.concatenate(
        [taper[:, None] * np.cos(angles), -taper[:, None] * np.sin(angles)], axis=1
    )
    factor = np.where(freqs == 0.0, 1.0, 2.0) / WINDOW
    synthesis = np.concatenate(
        [factor[:, None] * np.cos(angles).T, -factor[:, None] * np.sin(angles).T], axis=0
    )
    return analysis, synthesis


def banded(sources, places):
    analysis, synthesis = tables()
    strips = len(sources)
    forward = np.zeros((COEFS, LANE, strips, HOP))
    for n, s in enumerate(sources):
        if s < strips - 1:
            forward[:, s, n] = analysis[:HOP].T
        if s > 0:
            forward[:, s - 1, n] = analysis[HOP:].T
    backward = np.zeros((len(places), HOP, 2, MODES, LANE))
    for n, s in enumerate(places):
        backward[n, :, :, :, s] = synthesis[:, :HOP].T.reshape(HOP, 2, MODES)
        backward[n, :, :, :, s - 1] = synthesis[:, HOP:].T.reshape(HOP, 2, MODES)
    backward = backward.transpose(0, 1, 3, 2, 4)
    return (
        forward.reshape(COEFS * LANE, strips * HOP).astype(ml_dtypes.bfloat16),
        (0.5 * backward.reshape(len(places) * HOP, COEFS * LANE)).astype(ml_dtypes.bfloat16),
    )


def all_tables():
    sets = []
    for own, other, near, far in ((2, 4, 6, 0), (4, 2, 0, 6)):
        first = [p + n for p in (own, other, near, far) for n in range(2)]
        inner = first[:4] + [6 if p else 1 for p in (near, far)]
        second = [p - 1 for p in inner]
        sets.append(banded(first, inner) + banded(second, second[:4]))
    return [np.stack(t) for t in zip(*sets)]


def make_kernel(runs, n_in, edges):
    mid_rows = sum(len(run) - 2 for run in runs)
    out_rows = sum(len(run) - 4 for run in runs)

    def spans(cut):
        at = 0
        for run in runs:
            yield run, at, len(run) - cut
            at += len(run) - cut

    def kernel(info, *refs):
        bufs = refs[:n_in]
        spec, skip, diff, a1, s1, a2, s2 = refs[n_in : n_in + 7]
        outs = refs[n_in + 7 : n_in + 11]
        y, coef, mixed = refs[n_in + 11 :]
        high = info[0]
        core = info[1]
        near_inner = info[2]
        far_inner = info[3]

        def strips(row, *wanted):
            return [bufs[row[b][0]][e, row[b][1]] for b, e in wanted]

        evens = [(b, e) for b in range(4) for e in (core, 1 - core)]

        def window(row):
            return jnp.concatenate(strips(row, *evens), axis=0)

        def inner(row):
            return jnp.concatenate(
                strips(row, *evens[:4], (2, near_inner), (3, far_inner)), axis=0
            )

        def analyse(forward, rows):
            for r in range(0, len(rows), 2):
                two = [
                    jnp.dot(forward[high], get(), preferred_element_type=F32).reshape(
                        COEFS, LANE, 256
                    )
                    for get in rows[r : r + 2]
                ]
                coef[:, r * LANE : (r + 2) * LANE, :] = jnp.concatenate(two, axis=1).astype(BF16)

        def mix(l, rows):
            span = rows * LANE
            for k in range(MODES):
                re = coef[k, :span]
                im = coef[MODES + k, :span]
                wr = spec[l, 0, k]
                wi = spec[l, 1, k]
                parts = [
                    jnp.dot(
                        jnp.concatenate([re, i], axis=1),
                        jnp.concatenate(ws, axis=0),
                        preferred_element_type=F32,
                    ).reshape(rows, LANE, 256)
                    for i, ws in ((-im, (wr, wi)), (im, (wi, wr)))
                ]
                mixed[:rows, k * 2 * LANE : (k + 1) * 2 * LANE, :] = jnp.concatenate(
                    parts, axis=1
                ).astype(BF16)

        def synth(l, backward, get, at, rows, finish):
            local = skip[l] * 0.5
            spread = diff[l : l + 1] * 0.5
            lines = [get(r) for r in range(2)]
            wide = [v.astype(F32) for v in lines]
            for r in range(rows):
                lines.append(get(r + 2))
                wide.append(lines[r + 2].astype(F32))
                mid = wide[r + 1]
                total = jnp.dot(
                    lines[r + 1], local, preferred_element_type=F32
                ) + jnp.dot(backward[high], mixed[at + r], preferred_element_type=F32)
                half = total + spread * ((wide[r] - mid) + (wide[r + 2] - mid))
                inside = half * (GELU_A + GELU_B * (half * half))
                finish(at + r, ((mid + half) + half * jnp.tanh(inside)).astype(BF16))

        def first(r, value):
            y[r] = value

        def second(r, value):
            lower = core == 0
            for p in range(2):
                even = value[2 * p * HOP : (2 * p + 1) * HOP]
                odd = value[(2 * p + 1) * HOP : (2 * p + 2) * HOP]
                outs[2 * p][r] = jnp.where(lower, even, odd)
                outs[2 * p + 1][r] = jnp.where(lower, odd, even)

        analyse(a1, [lambda row=row: window(row) for run in runs for row in run[1:-1]])
        mix(0, mid_rows)
        for run, at, rows in spans(2):
            synth(0, s1, lambda r, run=run: inner(run[r]), at, rows, first)

        if edges:
            for n, row in enumerate((0, mid_rows - 1)):

                @pl.when(info[4 + n] == 1)
                def _(row=row):
                    y[row] = jnp.zeros((6 * HOP, 256), BF16)

        inside = [at + r for _, at, rows in spans(2) for r in range(1, rows - 1)]
        analyse(a2, [lambda r=r: y[r] for r in inside])
        mix(1, out_rows)
        for (_, at, rows), (_, start, _) in zip(spans(4), spans(2)):
            synth(1, s2, lambda r, start=start: y[start + r][: 4 * HOP], at, rows, second)

    vmem = pl.BlockSpec(memory_space=pltpu.VMEM)
    frames = 7 * mid_rows + 5 * out_rows
    return pl.pallas_call(
        kernel,
        out_shape=[jax.ShapeDtypeStruct((out_rows, HOP, 256), BF16)] * 4,
        in_specs=[pl.BlockSpec(memory_space=pltpu.SMEM)] + [vmem] * (n_in + 7),
        out_specs=[vmem] * 4,
        scratch_shapes=[
            pltpu.VMEM((mid_rows, 6 * HOP, 256), BF16),
            pltpu.VMEM((COEFS, mid_rows * LANE, 256), BF16),
            pltpu.VMEM((mid_rows, COEFS * LANE, 256), BF16),
        ],
        compiler_params=pltpu.CompilerParams(vmem_limit_bytes=VMEM_LIMIT),
        cost_estimate=pl.CostEstimate(
            flops=frames * (MODES * 8 * 256 * 256 + 2 * COEFS * (WINDOW + HOP) * 256),
            transcendentals=(mid_rows * 6 + out_rows * 4) * HOP * 256,
            bytes_accessed=mid_rows * 8 * HOP * 256 * 2,
        ),
        name="layers",
    )


def cut_middle(info, fields):
    shift, rows = MID

    def kernel(info, fields, *refs):
        outs, sem = refs[:6], refs[6]
        pos = info[0]
        copies = []
        for n, m in enumerate((2, 3, 1, 0)):
            src = fields.at[pl.ds((pos ^ m) * ROWS + shift, rows)]
            copies.append(pltpu.make_async_copy(src, outs[m], sem.at[n]))
        copies.append(pltpu.make_async_copy(fields.at[pl.ds(126, 2)], outs[4], sem.at[4]))
        copies.append(pltpu.make_async_copy(fields.at[pl.ds(0, 2)], outs[5], sem.at[5]))
        for c in copies:
            c.start()
        for c in copies:
            c.wait()

    vmem = pl.BlockSpec(memory_space=pltpu.VMEM)
    piece = jax.ShapeDtypeStruct((rows, HOP, 256), BF16)
    edge = jax.ShapeDtypeStruct((2, HOP, 256), BF16)
    return pl.pallas_call(
        kernel,
        out_shape=[piece] * 4 + [edge] * 2,
        in_specs=[
            pl.BlockSpec(memory_space=pltpu.SMEM),
            pl.BlockSpec(memory_space=pltpu.HBM),
        ],
        out_specs=[vmem] * 6,
        scratch_shapes=[pltpu.SemaphoreType.DMA((6,))],
        cost_estimate=pl.CostEstimate(flops=CUT_FLOPS, transcendentals=0, bytes_accessed=1 << 20),
        compiler_params=pltpu.CompilerParams(vmem_limit_bytes=SMALL_LIMIT),
        name="cut_middle",
    )(info, fields)


def cut_ends(info, fields, above, below):
    def kernel(info, fields, above, below, *refs):
        outs, sem = refs[:4], refs[4]
        pos = info[0]
        waits = []
        for m in (2, 3, 1, 0):
            block = pos ^ m
            start = block * ROWS
            out = outs[m]
            for n, (at, src, edge, beyond, other, last) in enumerate(
                (
                    (2, start, 0, start - 2, above, 0),
                    (END, start + ROWS - END + 2, 2 * END - 2, start + ROWS, below, 3),
                )
            ):
                c = pltpu.make_async_copy(
                    fields.at[pl.ds(src, END - 2)], out.at[pl.ds(at, END - 2)], sem.at[m, n, 0]
                )
                c.start()
                rim = out.at[pl.ds(edge, 2)]
                got = pltpu.make_async_copy(other, rim, sem.at[m, n, 1])

                @pl.when(block == last)
                def _(got=got):
                    got.start()

                @pl.when(block != last)
                def _(beyond=beyond, rim=rim, m=m, n=n):
                    pltpu.make_async_copy(
                        fields.at[pl.ds(beyond, 2)], rim, sem.at[m, n, 1]
                    ).start()

                waits += [c, got]
        for c in waits:
            c.wait()

    vmem = pl.BlockSpec(memory_space=pltpu.VMEM)
    piece = jax.ShapeDtypeStruct((2 * END, HOP, 256), BF16)
    return pl.pallas_call(
        kernel,
        out_shape=[piece] * 4,
        in_specs=[
            pl.BlockSpec(memory_space=pltpu.SMEM),
            pl.BlockSpec(memory_space=pltpu.HBM),
            pl.BlockSpec(memory_space=pl.ANY),
            pl.BlockSpec(memory_space=pl.ANY),
        ],
        out_specs=[vmem] * 4,
        scratch_shapes=[pltpu.SemaphoreType.DMA((4, 2, 2))],
        cost_estimate=pl.CostEstimate(flops=CUT_FLOPS, transcendentals=0, bytes_accessed=1 << 20),
        compiler_params=pltpu.CompilerParams(vmem_limit_bytes=SMALL_LIMIT),
        name="cut_ends",
    )(info, fields, above, below)


def paste(info, pieces, spots, result=None):
    def kernel(info, *refs):
        out, sem = refs[-2], refs[-1]
        copies = []
        for m in range(4):
            for n, (row, count, at) in enumerate(spots):
                dst = out.at[pl.ds((info[0] ^ m) * ROWS + at, count)]
                copies.append(
                    pltpu.make_async_copy(refs[m].at[pl.ds(row, count)], dst, sem.at[m, n])
                )
        for c in copies:
            c.start()
        for c in copies:
            c.wait()

    some = pl.BlockSpec(memory_space=pl.ANY)
    hbm = pl.BlockSpec(memory_space=pltpu.HBM)
    more = () if result is None else (result,)
    return pl.pallas_call(
        kernel,
        out_shape=jax.ShapeDtypeStruct((4 * ROWS, HOP, 256), BF16),
        in_specs=[pl.BlockSpec(memory_space=pltpu.SMEM)] + [some] * 4 + [hbm] * len(more),
        out_specs=hbm,
        input_output_aliases={5: 0} if more else {},
        scratch_shapes=[pltpu.SemaphoreType.DMA((4, len(spots)))],
        compiler_params=pltpu.CompilerParams(vmem_limit_bytes=SMALL_LIMIT),
        name="paste",
    )(info, *pieces, *more)


def load(spec_weight, skip_weight, diffusion, *tables):
    sources = (spec_weight, skip_weight, diffusion, *tables)
    count = len(sources)

    def kernel(*refs):
        sem = refs[2 * count]
        copies = [
            pltpu.make_async_copy(src, dst, sem.at[n])
            for n, (src, dst) in enumerate(zip(refs[:count], refs[count : 2 * count]))
        ]
        for c in copies:
            c.start()
        for c in copies:
            c.wait()

    return pl.pallas_call(
        kernel,
        out_shape=[pltpu.VMEM(v.shape, v.dtype) for v in sources],
        in_specs=[pl.BlockSpec(memory_space=pltpu.HBM)] * count,
        out_specs=[pl.BlockSpec(memory_space=pltpu.VMEM)] * count,
        scratch_shapes=[pltpu.SemaphoreType.DMA((count,))],
        compiler_params=pltpu.CompilerParams(vmem_limit_bytes=SMALL_LIMIT),
        name="load",
    )(*(pltpu.with_memory_space_constraint(v, pltpu.HBM) for v in sources))


def program(fields, spec_weight, skip_weight, diffusion):
    lon = lax.axis_index("lon")
    lat = lax.axis_index("lat")
    n_lon = lax.axis_size("lon")
    n_lat = lax.axis_size("lat")
    pos = lon % 4
    core = pos % 2

    def swap(v, m):
        return lax.ppermute(v, "lon", [(i, i ^ m) for i in range(n_lon)])

    def along(v, low, high):
        pairs = [(i, (i + (low if i % 4 < 2 else high)) % n_lon) for i in range(n_lon)]
        return lax.ppermute(v, "lon", pairs)

    info = jnp.stack(
        [
            pos // 2,
            core,
            jnp.where(pos < 2, core, 1 - core),
            jnp.where(pos < 2, 1 - core, core),
            ((lat == 0) & (pos == 0)).astype(jnp.int32),
            ((lat == n_lat - 1) & (pos == 3)).astype(jnp.int32),
        ]
    ).astype(jnp.int32)
    at = pos.astype(jnp.int32).reshape(1)

    own, one, two, three, tail, head = cut_middle(at, fields)
    above = lax.ppermute(tail, "lat", [(i, i + 1) for i in range(n_lat - 1)])
    below = lax.ppermute(head, "lat", [(i + 1, i) for i in range(n_lat - 1)])
    other_mid = jnp.stack([swap(two, 2), swap(three, 3)])
    own_mid = jnp.stack([own, swap(one, 1)])
    near_mid = along(own_mid, -4, 4)
    far_mid = along(other_mid, 4, -4)

    own, one, two, three = cut_ends(at, fields, above, below)
    other_end = jnp.stack([swap(two, 2), swap(three, 3)])
    own_end = jnp.stack([own, swap(one, 1)])
    near_end = along(own_end, -4, 4)
    far_end = along(other_end, 4, -4)

    mid = (own_mid, other_mid, near_mid, far_mid)
    end = (own_end, other_end, near_end, far_end)
    rest = load(spec_weight, skip_weight, diffusion, *map(jnp.asarray, all_tables()))

    def rows(first, start, count):
        return [[(first + b, r) for b in range(4)] for r in range(start, start + count)]

    outs = make_kernel([rows(0, 0, MID[1])], 4, False)(info, *mid, *rest)
    back_mid = [swap(outs[m], m) if m else outs[m] for m in range(4)]
    runs = [rows(0, 0, END) + rows(4, 0, 4), rows(4, MID[1] - 4, 4) + rows(0, END, END)]
    outs = make_kernel(runs, 8, True)(info, *end, *mid, *rest)
    back_end = [swap(outs[m], m) if m else outs[m] for m in range(4)]

    result = paste(at, back_mid, [(0, ROWS - 2 * END, END)])
    result = paste(at, back_end, [(0, END, 0), (END, END, ROWS - END)], result)
    return result


def solution(mesh):
    in_specs = (P("lat", "lon", None), P(), P(), P())
    out_specs = P("lat", "lon", None)
    return jax.shard_map(program, mesh=mesh, in_specs=in_specs, out_specs=out_specs, check_vma=False)
```
